128 devices in a mesh: rep: 1, dp: 128 (over x, y, z, core).
Axes of the slice: x: 4, y: 4, z: 4, core: 2. Of those that a mesh axis runs over, the one named last changes fastest.
Arguments:
- x: bfloat16 [128, 1024, 1280], P(('rep', 'dp'))
- dy: bfloat16 [128, 1024, 1280], P(('rep', 'dp'))
- w_gate: bfloat16 [2, 1280, 4096], replicated
- w_up: bfloat16 [2, 1280, 4096], replicated
- w_down: bfloat16 [2, 4096, 1280], replicated
- m_w_gate: float32 [2, 1280, 4096], P(None, 'dp')
- m_w_up: float32 [2, 1280, 4096], P(None, 'dp')
- m_w_down: float32 [2, 4096, 1280], P(None, 'dp')
- v_w_gate: float32 [2, 1280, 4096], P(None, 'dp')
- v_w_up: float32 [2, 1280, 4096], P(None, 'dp')
- v_w_down: float32 [2, 4096, 1280], P(None, 'dp')
Outputs:
- output 1: bfloat16 [2, 1280, 4096], P('rep')
- output 2: bfloat16 [2, 1280, 4096], P('rep')
- output 3: bfloat16 [2, 4096, 1280], P('rep')
- output 4: float32 [2, 1280, 4096], P('rep', 'dp')
- output 5: float32 [2, 1280, 4096], P('rep', 'dp')
- output 6: float32 [2, 4096, 1280], P('rep', 'dp')
- output 7: float32 [2, 1280, 4096], P('rep', 'dp')
- output 8: float32 [2, 1280, 4096], P('rep', 'dp')
- output 9: float32 [2, 4096, 1280], P('rep', 'dp')
All inputs are finite; a program needn't handle non-finite values.
Results may differ from the reference program's by a relative error of at most 0.022.
Values are sent between devices in bfloat16 or wider.
A program may use at most 1.5 GiB of HBM per device.

```python
import jax
import jax.numpy as jnp
from jax import lax

SEQUENCES = 128
TOKENS = 1024
D = 1280
FF = 4096
LAYERS = 2
NAMES = ("w_gate", "w_up", "w_down")
SHAPES = {"w_gate": (LAYERS, D, FF), "w_up": (LAYERS, D, FF), "w_down": (LAYERS, FF, D)}


def bump(key, n, height):
    away = (jnp.arange(n, dtype=jnp.int32) - jax.random.randint(key, (), 0, n, jnp.int32)) % n
    return jnp.where(away < n // 8, height, 1.0)


def together(key, own, strength):
    shared = jax.random.normal(key, own.shape[1:], jnp.float32)
    return (own + strength * shared) * lax.rsqrt(1 + strength * strength)


def setup_inputs(seed: int = 0, part: int = 0) -> dict:
    kx, kdy, ka, kb, kz, kf, kh, kl, *keys = jax.random.split(jax.random.key(seed), 8 + 3 * len(NAMES))
    kx, kdy, ka, kb = (jax.random.fold_in(k, part) for k in (kx, kdy, ka, kb))
    kw, km, kv = (keys[i::3] for i in range(3))
    shape = (SEQUENCES, TOKENS, D)
    much_x, much_dy = jax.random.uniform(kz, (2,), jnp.float32, 0.0, 1.0)
    loud = 2.0 ** jax.random.uniform(jax.random.fold_in(kz, 1), (), jnp.float32, -1.0, 2.0)
    layers = 2.0 ** jax.random.uniform(kl, (LAYERS, 1, 1), jnp.float32, -1.0, 1.0)
    x = together(ka, jax.random.normal(kx, shape, jnp.float32), much_x) * bump(kf, D, 4.0)
    dy = together(kb, jax.random.normal(kdy, shape, jnp.float32), much_dy)
    drawn = {"x": x.astype(jnp.bfloat16), "dy": (loud * dy * (SEQUENCES * TOKENS) ** -0.5).astype(jnp.bfloat16)}
    for key, name in zip(kw, NAMES, strict=True):
        w = jax.random.normal(key, SHAPES[name], jnp.float32) * SHAPES[name][1] ** -0.5
        drawn[name] = (w * {"w_gate": 1.0, "w_up": bump(kh, FF, 4.0), "w_down": layers}[name]).astype(jnp.bfloat16)
    for key, name in zip(km, NAMES, strict=True):
        drawn[f"m_{name}"] = 0.1 * jax.random.normal(key, SHAPES[name], jnp.float32)
    for key, name in zip(kv, NAMES, strict=True):
        drawn[f"v_{name}"] = loud * loud * jax.random.uniform(key, SHAPES[name], jnp.float32, 0.05, 0.15)
    return drawn


def matmul(a, w):
    return jnp.dot(a, w, preferred_element_type=jnp.float32).astype(jnp.bfloat16)


def normed(h):
    wide = h.astype(jnp.float32)
    scale = lax.rsqrt(jnp.mean(wide**2, -1, keepdims=True) + 1e-6)
    return (wide * scale).astype(jnp.bfloat16)


def layer(h, w):
    a = normed(h)
    gate = jnp.dot(a, w["w_gate"], preferred_element_type=jnp.float32)
    up = jnp.dot(a, w["w_up"], preferred_element_type=jnp.float32)
    return h + matmul((jax.nn.silu(gate) * up).astype(jnp.bfloat16), w["w_down"])


def adamw(w, m, v, g):
    m = 0.9 * m + 0.1 * g
    v = 0.95 * v + 0.05 * g * g
    step = m * lax.rsqrt(v + 1e-8) + 0.1 * w
    return (w - 0.02 * step).astype(jnp.bfloat16), m, v


def stack(weights, h):
    return lax.scan(lambda h, w: (layer(h, w), None), h, weights)[0]


def reference(x, dy, w_gate, w_up, w_down, m_w_gate, m_w_up, m_w_down, v_w_gate, v_w_up, v_w_down):
    weights = dict(zip(NAMES, (w_gate, w_up, w_down), strict=True))

    def take(so_far, sequence):
        h, by_y = sequence
        _, back = jax.vjp(lambda w: stack(w, h), weights)
        return jax.tree.map(lambda total, term: total + term.astype(jnp.float32), so_far, back(by_y)[0]), None

    none_yet = {name: jnp.zeros(w.shape, jnp.float32) for name, w in weights.items()}
    by_weights, _ = lax.scan(take, none_yet, (x, dy))
    gradients = [by_weights[name].astype(jnp.bfloat16).astype(jnp.float32) for name in NAMES]
    new = [
        adamw(w.astype(jnp.float32), m, v, g)
        for w, m, v, g in zip((w_gate, w_up, w_down), (m_w_gate, m_w_up, m_w_down), (v_w_gate, v_w_up, v_w_down), gradients, strict=True)
    ]
    return tuple(one[which] for which in range(3) for one in new)
```

```python
import jax
import jax.numpy as jnp
from jax import lax
from jax.sharding import PartitionSpec as P


BF = jnp.bfloat16
F32 = jnp.float32
GRID = [(x, y, z, c) for x in range(4) for y in range(4) for z in range(4) for c in range(2)]


def number(x, y, z, c):
    return (((x % 4) * 4 + y % 4) * 4 + z % 4) * 2 + c % 2


def shift(axis, by):
    moved = {"x": (1, 0, 0, 0), "y": (0, 1, 0, 0), "z": (0, 0, 1, 0), "c": (0, 0, 0, 1)}[axis]
    return [(number(*p), number(*(a + by * b for a, b in zip(p, moved)))) for p in GRID]


def spread(j):
    pairs = []
    for x, y, z, c in GRID:
        k = (z + j) % 4
        pairs.append((number(x, y, z, c), number(x, y, 2 * c + k // 2, k % 2)))
    return pairs


def send(a, pairs):
    return lax.ppermute(a, "dp", pairs)


def at(a, i, axis):
    return lax.dynamic_index_in_dim(a, i, axis, keepdims=False)


def total(terms):
    out = terms[0].astype(F32)
    for t in terms[1:]:
        out = out + t.astype(F32)
    return out


def scatter_stage(terms, axis, name, place):
    got = []
    for by in (1, 3, 2):
        part = total([at(t, (place + by) % 4, axis) for t in terms]).astype(BF)
        got.append(send(part, shift(name, by)))
    return [at(t, place, axis) for t in terms] + got


def gather_stage(own, axis, name, place):
    parts = [own] + [send(own, shift(name, -by)) for by in (1, 2, 3)]
    twice = jnp.stack(parts + parts[:3], axis)
    return lax.dynamic_slice_in_dim(twice, (4 - place) % 4, 4, axis)


def adamw(w, m, v, g):
    m = 0.9 * m + 0.1 * g
    v = 0.95 * v + 0.05 * g * g
    step = m * lax.rsqrt(v + 1e-8) + 0.1 * w
    return (w - 0.02 * step).astype(BF), m, v


def matmul(a, w):
    return jnp.dot(a, w, preferred_element_type=F32).astype(BF)


def normed(h):
    wide = h.astype(F32)
    scale = lax.rsqrt(jnp.mean(wide**2, -1, keepdims=True) + 1e-6)
    return (wide * scale).astype(BF)


def layer(h, wg, wu, wd):
    a = normed(h)
    gate = jnp.dot(a, wg, preferred_element_type=F32)
    up = jnp.dot(a, wu, preferred_element_type=F32)
    return h + matmul((jax.nn.silu(gate) * up).astype(BF), wd)


def solution(mesh):
    def body(x, dy, wg, wu, wd, mg, mu, md, vg, vu, vd):
        me = lax.axis_index("dp")
        px, py, pz, pc = me // 32, me // 8 % 4, me // 2 % 4, me % 2
        h, by_y = x[0], dy[0]

        def scatter_wide(g, first):
            g = g.reshape(4, 4, 2, 40, 4096)
            r = send(at(g, 1 - pc, 2), shift("c", 1))
            terms = [at(g, pc, 2), r]
            if first == "x":
                terms = scatter_stage(terms, 0, "x", px)
                terms = scatter_stage(terms, 0, "y", py)
            else:
                terms = scatter_stage(terms, 1, "y", py)
                terms = scatter_stage(terms, 0, "x", px)
            mine = total(terms).reshape(4, 10, 4096)
            out = jnp.zeros((10, 4096), F32)
            for j in range(4):
                k = (pz + j) % 4
                block = at(mine, k, 0)
                got = send(block.astype(BF), spread(j)).astype(F32)
                stays = (2 * pc + k // 2 == pz) & (k % 2 == pc)
                out = out + jnp.where(stays, block, got)
            return out

        def scatter_tall(g, order):
            g = g.reshape(4, 4, 4, 2, 32, 1280)
            r = send(at(g, 1 - pc, 3), shift("c", 1))
            terms = scatter_stage([at(g, pc, 3), r], 2, "z", pz)
            terms = scatter_stage(terms, 0, "x", px)
            terms = scatter_stage(terms, 0, "y", py)
            return total(terms)

        def pieces(s, name):
            parts = [(0, s)] + [(by, send(s, shift(name, -by))) for by in (1, 3, 2)]
            return [(by, 0, t) for by, t in parts] + [(by, 1, send(t, shift("c", 1))) for by, t in parts]

        def gather_wide(w, last, out, n):
            got = [send(w, [(b, a) for a, b in spread(j)]) for j in range(4)]
            twice = jnp.stack(got + got[:3])
            w = lax.dynamic_slice_in_dim(twice, (4 - pz) % 4, 4, 0).reshape(40, 4096)
            if last == "x":
                w = gather_stage(w, 0, "y", py)
                for by, other, t in pieces(w, "x"):
                    t = t[None, None, :, None]
                    out = lax.dynamic_update_slice(out, t, (n, (px + by) % 4, 0, pc ^ other, 0, 0))
            else:
                w = gather_stage(w, 0, "x", px)
                for by, other, t in pieces(w, "y"):
                    t = t[None, :, None, None]
                    out = lax.dynamic_update_slice(out, t, (n, 0, (py + by) % 4, pc ^ other, 0, 0))
            return out

        def gather_tall(w, out, n):
            w = gather_stage(w, 0, "y", py)
            w = gather_stage(w, 0, "x", px)
            for by, other, t in pieces(w, "z"):
                t = t[None, :, :, None, None]
                out = lax.dynamic_update_slice(out, t, (n, 0, 0, (pz + by) % 4, pc ^ other, 0, 0))
            return out

        h1, back0 = jax.vjp(lambda *w: layer(h, *w), wg[0], wu[0], wd[0])
        _, back1 = jax.vjp(layer, h1, wg[1], wu[1], wd[1])
        by_h1, *by_1 = back1(by_y)
        by_0 = back0(by_h1)

        outs = [jnp.zeros((2, 4, 4, 2, 40, 4096), BF), jnp.zeros((2, 4, 4, 2, 40, 4096), BF), jnp.zeros((2, 4, 4, 4, 2, 32, 1280), BF)]
        new_m, new_v = {}, {}
        for n, (g_g, g_u, g_d) in ((1, by_1), (0, by_0)):
            sums = (scatter_wide(g_g, "x"), scatter_wide(g_u, "y"), scatter_tall(g_d, None))
            for i, (g, w, m, v) in enumerate(zip(sums, (wg, wu, wd), (mg, mu, md), (vg, vu, vd))):
                rows = g.shape[0]
                own = lax.dynamic_slice_in_dim(w[n], me * rows, rows, 0).astype(F32)
                w_new, new_m[i, n], new_v[i, n] = adamw(own, m[n], v[n], g.astype(BF).astype(F32))
                if i == 2:
                    outs[i] = gather_tall(w_new, outs[i], n)
                else:
                    outs[i] = gather_wide(w_new, "xy"[i], outs[i], n)
        weights = [o.reshape(w.shape) for o, w in zip(outs, (wg, wu, wd))]
        stacked = [[jnp.stack([t[i, n] for n in range(2)]) for i in range(3)] for t in (new_m, new_v)]
        return (*weights, *stacked[0], *stacked[1])

    rows = P(None, "dp", None)
    return jax.shard_map(
        body,
        mesh=mesh,
        in_specs=(P("dp"), P("dp"), P(), P(), P(), *[rows] * 6),
        out_specs=(P(), P(), P(), *[rows] * 6),
        check_vma=False,
    )
```

```python
import jax
import jax.numpy as jnp
from jax import lax
from jax.experimental import pallas as pl
from jax.experimental.pallas import tpu as pltpu
from jax.sharding import PartitionSpec as P


MESH = pl.DeviceIdType.MESH
BF = jnp.bfloat16
F32 = jnp.float32
GRID = [(x, y, z, c) for x in range(4) for y in range(4) for z in range(4) for c in range(2)]


def number(x, y, z, c):
    return (((x % 4) * 4 + y % 4) * 4 + z % 4) * 2 + c % 2


def shift(axis, by):
    moved = {"x": (1, 0, 0, 0), "y": (0, 1, 0, 0), "z": (0, 0, 1, 0), "c": (0, 0, 0, 1)}[axis]
    return [(number(*p), number(*(a + by * b for a, b in zip(p, moved)))) for p in GRID]


def spread(j):
    pairs = []
    for x, y, z, c in GRID:
        k = (z + j) % 4
        pairs.append((number(x, y, z, c), number(x, y, 2 * c + k // 2, k % 2)))
    return pairs


def send(a, pairs):
    return lax.ppermute(a, "dp", pairs)


def at(a, i, axis):
    return lax.dynamic_index_in_dim(a, i, axis, keepdims=False)


def total(terms):
    out = terms[0].astype(F32)
    for t in terms[1:]:
        out = out + t.astype(F32)
    return out


def scatter_stage(terms, axis, name, place):
    got = []
    for by in (1, 3, 2):
        part = total([at(t, (place + by) % 4, axis) for t in terms]).astype(BF)
        got.append(send(part, shift(name, by)))
    return [at(t, place, axis) for t in terms] + got


def gather_stage(own, axis, name, place):
    parts = [own] + [send(own, shift(name, -by)) for by in (1, 2, 3)]
    twice = jnp.stack(parts + parts[:3], axis)
    return lax.dynamic_slice_in_dim(twice, (4 - place) % 4, 4, axis)


KINDS = ("zyx", "xzy", "yxz")


def neighbour(axis, by):
    me = lax.axis_index("dp")
    here = {"x": me // 32, "y": me // 8 % 4, "z": me // 2 % 4, "c": me % 2}
    size = 2 if axis == "c" else 4
    here[axis] = lax.rem(here[axis] + by, size)
    return {"dp": ((here["x"] * 4 + here["y"]) * 4 + here["z"]) * 2 + here["c"]}


PEERS = [(a, by) for a in "xyz" for by in (1, 2, 3)] + [("c", 1)]


def greet():
    barrier = pltpu.get_barrier_semaphore()
    for axis, by in PEERS:
        pl.semaphore_signal(barrier, inc=1, device_id=neighbour(axis, by), device_id_type=MESH)
    pl.semaphore_wait(barrier, len(PEERS))


def gather_kernel(own_g, own_u, own_d, out_g, out_u, out_d, local_sem, send_sem, recv_sem):
    me = lax.axis_index("dp")
    here = {"x": me // 32, "y": me // 8 % 4, "z": me // 2 % 4}
    c = me % 2
    greet()
    owns, outs = (own_g, own_u, own_d), (out_g, out_u, out_d)
    started = []

    def view(k, **where):
        spots = [where.get(a, slice(None)) for a in "xyz"]
        return outs[k].at[(slice(None), *spots, c)]

    def push(src, dst, axis, by):
        n = len(started)
        copy = pltpu.make_async_remote_copy(
            src_ref=src, dst_ref=dst, send_sem=send_sem.at[n], recv_sem=recv_sem.at[n], device_id=neighbour(axis, by), device_id_type=MESH
        )
        copy.start()
        started.append(copy)
        return copy

    first, second, third, relay, swaps = {}, {}, {}, {}, []
    keep = []
    for k in range(3):
        local = pltpu.make_async_copy(owns[k], view(k, **here), local_sem.at[k])
        local.start()
        keep.append(local)
        first[k] = [push(owns[k], view(k, **here), KINDS[k][0], by) for by in (1, 3, 2)]
    for k, (a, b, e) in enumerate(KINDS):
        keep[k].wait()
        for copy in first[k]:
            copy.wait_recv()
        line = view(k, **{b: here[b], e: here[e]})
        second[k] = [push(line, line, b, by) for by in (1, 3, 2)]
    for k, (a, b, e) in enumerate(KINDS):
        for copy in second[k]:
            copy.wait_recv()
        plane = view(k, **{e: here[e]})
        third[k] = [push(plane, plane, e, by) for by in (1, 3)]
        swaps.append(push(plane, plane, "c", 1))
    for k, (a, b, e) in enumerate(KINDS):
        relay[k] = []
        for copy, by, half in zip(third[k], (1, 3), (slice(0, 2), slice(2, 4))):
            copy.wait_recv()
            came = lax.rem(here[e] + 4 - by, 4)
            part = view(k, **{e: came, a: half})
            relay[k].append(push(part, part, e, by))
            plane = view(k, **{e: came})
            swaps.append(push(plane, plane, "c", 1))
    for k, (a, b, e) in enumerate(KINDS):
        for copy, half in zip(relay[k], (slice(0, 2), slice(2, 4))):
            copy.wait_recv()
            part = view(k, **{e: lax.rem(here[e] + 2, 4), a: half})
            swaps.append(push(part, part, "c", 1))
    for copy in swaps:
        copy.wait_recv()
    for copy in started:
        copy.wait_send()


COPIES = 3 * (3 + 3 + 2 + 2 + 5)


def gather(owns):
    shapes = [jax.ShapeDtypeStruct((2, 4, 4, 4, 2, *o.shape[1:]), o.dtype) for o in owns]
    return pl.pallas_call(
        gather_kernel,
        out_shape=shapes,
        in_specs=[pl.BlockSpec(memory_space=pltpu.VMEM)] * 3,
        out_specs=[pl.BlockSpec(memory_space=pl.ANY)] * 3,
        scratch_shapes=[pltpu.SemaphoreType.DMA((3,)), pltpu.SemaphoreType.DMA((COPIES,)), pltpu.SemaphoreType.DMA((COPIES,))],
        compiler_params=pltpu.CompilerParams(collective_id=0, has_side_effects=True),
        name="gather",
    )(*owns)


def adamw(w, m, v, g):
    m = 0.9 * m + 0.1 * g
    v = 0.95 * v + 0.05 * g * g
    step = m * lax.rsqrt(v + 1e-8) + 0.1 * w
    return (w - 0.02 * step).astype(BF), m, v


def matmul(a, w):
    return jnp.dot(a, w, preferred_element_type=F32).astype(BF)


def normed(h):
    wide = h.astype(F32)
    scale = lax.rsqrt(jnp.mean(wide**2, -1, keepdims=True) + 1e-6)
    return (wide * scale).astype(BF)


def layer(h, wg, wu, wd):
    a = normed(h)
    gate = jnp.dot(a, wg, preferred_element_type=F32)
    up = jnp.dot(a, wu, preferred_element_type=F32)
    return h + matmul((jax.nn.silu(gate) * up).astype(BF), wd)


def solution(mesh):
    def body(x, dy, wg, wu, wd, mg, mu, md, vg, vu, vd):
        me = lax.axis_index("dp")
        px, py, pz, pc = me // 32, me // 8 % 4, me // 2 % 4, me % 2
        h, by_y = x[0], dy[0]

        def scatter_wide(g, first):
            g = g.reshape(4, 4, 2, 40, 4096)
            r = send(at(g, 1 - pc, 2), shift("c", 1))
            terms = [at(g, pc, 2), r]
            if first == "x":
                terms = scatter_stage(terms, 0, "x", px)
                terms = scatter_stage(terms, 0, "y", py)
            else:
                terms = scatter_stage(terms, 1, "y", py)
                terms = scatter_stage(terms, 0, "x", px)
            mine = total(terms).reshape(4, 10, 4096)
            out = jnp.zeros((10, 4096), F32)
            for j in range(4):
                k = (pz + j) % 4
                block = at(mine, k, 0)
                got = send(block.astype(BF), spread(j)).astype(F32)
                stays = (2 * pc + k // 2 == pz) & (k % 2 == pc)
                out = out + jnp.where(stays, block, got)
            return out

        def scatter_tall(g, order):
            g = g.reshape(4, 4, 4, 2, 32, 1280)
            r = send(at(g, 1 - pc, 3), shift("c", 1))
            terms = scatter_stage([at(g, pc, 3), r], 2, "z", pz)
            terms = scatter_stage(terms, 0, "x", px)
            terms = scatter_stage(terms, 0, "y", py)
            return total(terms)

        h1, back0 = jax.vjp(lambda *w: layer(h, *w), wg[0], wu[0], wd[0])
        _, back1 = jax.vjp(layer, h1, wg[1], wu[1], wd[1])
        by_h1, *by_1 = back1(by_y)
        by_0 = back0(by_h1)

        new = {}
        for n, (g_g, g_u, g_d) in ((1, by_1), (0, by_0)):
            sums = (scatter_wide(g_g, "x"), scatter_wide(g_u, "y"), scatter_tall(g_d, None))
            for i, (g, w, m, v) in enumerate(zip(sums, (wg, wu, wd), (mg, mu, md), (vg, vu, vd))):
                rows = g.shape[0]
                own = lax.dynamic_slice_in_dim(w[n], me * rows, rows, 0).astype(F32)
                new[i, n] = adamw(own, m[n], v[n], g.astype(BF).astype(F32))
        stacked = [[jnp.stack([new[i, n][which] for n in range(2)]) for i in range(3)] for which in range(3)]
        owns = [stacked[0][0].reshape(2, 320, 128), stacked[0][1].reshape(2, 320, 128), stacked[0][2]]
        weights = [o.reshape(w.shape) for o, w in zip(gather(owns), (wg, wu, wd))]
        return (*weights, *stacked[1], *stacked[2])

    rows = P(None, "dp", None)
    return jax.shard_map(
        body,
        mesh=mesh,
        in_specs=(P("dp"), P("dp"), P(), P(), P(), *[rows] * 6),
        out_specs=(P(), P(), P(), *[rows] * 6),
        check_vma=False,
    )
```

```python
import functools

import jax
import jax.numpy as jnp
from jax import lax
from jax.experimental import pallas as pl
from jax.experimental.pallas import tpu as pltpu
from jax.sharding import PartitionSpec as P

MESH = pl.DeviceIdType.MESH
BF = jnp.bfloat16
F32 = jnp.float32


KINDS = ("zyx", "xzy", "yxz")


def neighbour(axis, by):
    me = lax.axis_index("dp")
    here = {"x": me // 32, "y": me // 8 % 4, "z": me // 2 % 4, "c": me % 2}
    size = 2 if axis == "c" else 4
    here[axis] = lax.rem(here[axis] + by, size)
    return {"dp": ((here["x"] * 4 + here["y"]) * 4 + here["z"]) * 2 + here["c"]}


PEERS = [(a, by) for a in "xyz" for by in (1, 2, 3)] + [("c", 1)]


def greet():
    barrier = pltpu.get_barrier_semaphore()
    for axis, by in PEERS:
        pl.semaphore_signal(barrier, inc=1, device_id=neighbour(axis, by), device_id_type=MESH)
    pl.semaphore_wait(barrier, len(PEERS))


def gather_kernel(own_g, own_u, own_d, out_g, out_u, out_d, local_sem, send_sem, recv_sem):
    me = lax.axis_index("dp")
    here = {"x": me // 32, "y": me // 8 % 4, "z": me // 2 % 4}
    c = me % 2
    greet()
    owns, outs = (own_g, own_u, own_d), (out_g, out_u, out_d)
    started = []

    def view(k, **where):
        spots = [where.get(a, slice(None)) for a in "xyz"]
        return outs[k].at[(slice(None), *spots, c)]

    def push(src, dst, axis, by):
        n = len(started)
        copy = pltpu.make_async_remote_copy(
            src_ref=src, dst_ref=dst, send_sem=send_sem.at[n], recv_sem=recv_sem.at[n], device_id=neighbour(axis, by), device_id_type=MESH
        )
        copy.start()
        started.append(copy)
        return copy

    first, second, third, relay, swaps = {}, {}, {}, {}, []
    keep = []
    for k in range(3):
        local = pltpu.make_async_copy(owns[k], view(k, **here), local_sem.at[k])
        local.start()
        keep.append(local)
        first[k] = [push(owns[k], view(k, **here), KINDS[k][0], by) for by in (1, 3, 2)]
    for k, (a, b, e) in enumerate(KINDS):
        keep[k].wait()
        for copy in first[k]:
            copy.wait_recv()
        line = view(k, **{b: here[b], e: here[e]})
        second[k] = [push(line, line, b, by) for by in (1, 3, 2)]
    for k, (a, b, e) in enumerate(KINDS):
        for copy in second[k]:
            copy.wait_recv()
        plane = view(k, **{e: here[e]})
        third[k] = [push(plane, plane, e, by) for by in (1, 3)]
        swaps.append(push(plane, plane, "c", 1))
    for k, (a, b, e) in enumerate(KINDS):
        relay[k] = []
        for copy, by, half in zip(third[k], (1, 3), (slice(0, 2), slice(2, 4))):
            copy.wait_recv()
            came = lax.rem(here[e] + 4 - by, 4)
            part = view(k, **{e: came, a: half})
            relay[k].append(push(part, part, e, by))
            plane = view(k, **{e: came})
            swaps.append(push(plane, plane, "c", 1))
    for k, (a, b, e) in enumerate(KINDS):
        for copy, half in zip(relay[k], (slice(0, 2), slice(2, 4))):
            copy.wait_recv()
            part = view(k, **{e: lax.rem(here[e] + 2, 4), a: half})
            swaps.append(push(part, part, "c", 1))
    for copy in swaps:
        copy.wait_recv()
    for copy in started:
        copy.wait_send()


COPIES = 3 * (3 + 3 + 2 + 2 + 5)


def gather(owns):
    shapes = [jax.ShapeDtypeStruct((2, 4, 4, 4, 2, *o.shape[1:]), o.dtype) for o in owns]
    return pl.pallas_call(
        gather_kernel,
        out_shape=shapes,
        in_specs=[pl.BlockSpec(memory_space=pltpu.VMEM)] * 3,
        out_specs=[pl.BlockSpec(memory_space=pl.ANY)] * 3,
        scratch_shapes=[pltpu.SemaphoreType.DMA((3,)), pltpu.SemaphoreType.DMA((COPIES,)), pltpu.SemaphoreType.DMA((COPIES,))],
        compiler_params=pltpu.CompilerParams(collective_id=0, has_side_effects=True),
        name="gather",
    )(*owns)


def place():
    me = lax.axis_index("dp")
    return me // 32, me // 8 % 4, me // 2 % 4, me % 2


def combine(dst, terms):
    *lead, rows, _ = dst.shape
    strips = rows // 16
    count = strips
    for n in lead:
        count *= n

    @pl.loop(0, count)
    def _(i):
        spot, q = [], i // strips
        for n in reversed(lead):
            spot.insert(0, q % n)
            q = q // n
        where = (*spot, pl.ds(pl.multiple_of(i % strips * 16, 16), 16), slice(None))
        out = terms[0][where].astype(F32)
        for t in terms[1:]:
            out = out + t[where].astype(F32)
        dst[where] = out.astype(dst.dtype)


def transposed_product(a, b, out, rows, columns):
    depth = a.shape[0]

    def tile(a_ref, b_ref, o_ref):
        o_ref[...] = lax.dot_general(a_ref[...], b_ref[...], (((0,), (0,)), ((), ())), preferred_element_type=F32).astype(BF)

    pltpu.emit_pipeline(
        tile,
        grid=(a.shape[1] // rows, b.shape[1] // columns),
        in_specs=[pl.BlockSpec((depth, rows), lambda i, j: (0, i)), pl.BlockSpec((depth, columns), lambda i, j: (0, j))],
        out_specs=[pl.BlockSpec((rows, columns), lambda i, j: (i, j))],
    )(a, b, out)


STEPS = (0, 1, 2)
BYS = (1, 3, 2)


def scatter_kernel(beside, g_g, g_u, g_d, *rest):
    ins, rest = rest[: 2 * beside], rest[2 * beside :]
    f_g, f_u, f_d = rest[:3]
    products, rest = rest[3 : 3 + beside], rest[3 + beside :]
    o_g, r_g, p_g, q_g, o_u, r_u, p_u, q_u, o_d, r_d, p_d, q_d, t_d, local_sem, send_sem, recv_sem = rest
    px, py, pz, pc = place()
    greet()
    started = []

    def push(src, dst, axis, by):
        n = len(started)
        copy = pltpu.make_async_remote_copy(
            src_ref=src, dst_ref=dst, send_sem=send_sem.at[n], recv_sem=recv_sem.at[n], device_id=neighbour(axis, by), device_id_type=MESH
        )
        copy.start()
        started.append(copy)
        return copy

    def half(k, c):
        if k == 2:
            return g_d.at[:, :, :, c]
        return (g_g, g_u)[k].at[:, :, :, pl.ds(pl.multiple_of(c * 2048, 2048), 2048)]

    own, swapped = (o_g, o_u, o_d), (r_g, r_u, r_d)
    firsts, seconds = (p_g, p_u, p_d), (q_g, q_u, q_d)
    axes = ("xy", "yx", "zx")
    here = {"x": px, "y": py, "z": pz}

    def first_part(k, ref, t):
        return (ref.at[t], ref.at[:, t], ref.at[:, :, t])[k]

    def second_part(k, ref, t):
        return (ref.at[px, t], ref.at[t, py], ref.at[t, :, pz])[k]

    swaps, loads = [], []
    for k in range(3):
        swaps.append(push(half(k, 1 - pc), swapped[k], "c", 1))
        loads.append(pltpu.make_async_copy(half(k, pc), own[k], local_sem.at[k]))
        loads[k].start()

    def product(n):
        if n < beside:
            transposed_product(ins[2 * n], ins[2 * n + 1], products[n], *((512, 1280) if n == 0 else (640, 1024)))

    ring = {}
    for k in range(3):
        loads[k].wait()
        swaps[k].wait_recv()
        ring[k] = []
        for i, by in enumerate(BYS):
            t = lax.rem(here[axes[k][0]] + by, 4)
            part = first_part(k, own[k], t)
            combine(part, [part, first_part(k, swapped[k], t)])
            ring[k].append(push(part, firsts[k].at[i], axes[k][0], by))
    for n in STEPS:
        product(n)
    ring2 = {}
    for k in range(3):
        for copy in ring[k]:
            copy.wait_recv()
        ring2[k] = []
        for i, by in enumerate(BYS):
            t = lax.rem(here[axes[k][1]] + by, 4)
            part = second_part(k, own[k], t)
            combine(part, [part, second_part(k, swapped[k], t)] + [firsts[k].at[s, t] for s in STEPS])
            ring2[k].append(push(part, seconds[k].at[i], axes[k][1], by))
    last = []
    for copy in ring2[2]:
        copy.wait_recv()

    def terms_d(u):
        return [o_d.at[px, u, pz], r_d.at[px, u, pz]] + [p_d.at[s, px, u] for s in STEPS] + [q_d.at[s, u] for s in STEPS]

    for i, by in enumerate(BYS):
        u = lax.rem(py + by, 4)
        combine(o_d.at[px, u, pz], terms_d(u))
        last.append(push(o_d.at[px, u, pz], t_d.at[i], "y", by))
    for k, f in ((0, f_g), (1, f_u)):
        for copy in ring2[k]:
            copy.wait_recv()
        t = here[axes[k][1]]
        combine(f, [second_part(k, own[k], t), second_part(k, swapped[k], t)] + [firsts[k].at[s, t] for s in STEPS] + [seconds[k].at[s] for s in STEPS])
    for copy in last:
        copy.wait_recv()
    combine(f_d, terms_d(py) + [t_d.at[s] for s in STEPS])
    for copy in started:
        copy.wait_send()


def scatter(g_g, g_u, g_d, beside, identity):
    any_space, vmem = pl.BlockSpec(memory_space=pl.ANY), pl.BlockSpec(memory_space=pltpu.VMEM)
    copies = 3 + 9 + 9 + 3
    wide, tall = (4, 80, 2048), (4, 32, 1280)
    shapes = []
    for _ in range(2):
        shapes += [(4, *wide), (4, *wide), (3, *wide), (3, *wide[1:])]
    shapes += [(4, 4, *tall), (4, 4, *tall), (3, 4, *tall), (3, *tall), (3, *tall[1:])]
    operands = [t for pair in beside for t in pair]
    out = pl.pallas_call(
        functools.partial(scatter_kernel, len(beside)),
        out_shape=[jax.ShapeDtypeStruct((80, 2048), F32)] * 2
        + [jax.ShapeDtypeStruct((32, 1280), F32)]
        + [jax.ShapeDtypeStruct((a.shape[1], b.shape[1]), BF) for a, b in beside],
        in_specs=[any_space] * (3 + len(operands)),
        out_specs=[vmem] * 3 + [any_space] * len(beside),
        scratch_shapes=[pltpu.VMEM(s, BF) for s in shapes]
        + [pltpu.SemaphoreType.DMA((3,)), pltpu.SemaphoreType.DMA((copies,)), pltpu.SemaphoreType.DMA((copies,))],
        compiler_params=pltpu.CompilerParams(collective_id=identity, has_side_effects=True, vmem_limit_bytes=66_000_000),
        name=f"scatter{identity}",
    )(g_g.reshape(4, 4, 80, 4096), g_u.reshape(4, 4, 80, 4096), g_d.reshape(4, 4, 4, 2, 32, 1280), *operands)
    return out[:3], out[3:]


COLUMN = [(dz, dc) for dz in range(4) for dc in range(2) if dz or dc]


def column_kernel(parts, kept, out, came, send_sem, recv_sem):
    px, py, pz, pc = place()

    def peer(dz, dc):
        return {"dp": ((px * 4 + py) * 4 + lax.rem(pz + dz, 4)) * 2 + lax.rem(pc + dc, 2)}

    barrier = pltpu.get_barrier_semaphore()
    for dz, dc in COLUMN:
        pl.semaphore_signal(barrier, inc=1, device_id=peer(dz, dc), device_id_type=MESH)
    pl.semaphore_wait(barrier, len(COLUMN))
    copies = []
    for n, (dz, dc) in enumerate(COLUMN):
        copy = pltpu.make_async_remote_copy(
            src_ref=parts.at[lax.rem(pz + dz, 4), lax.rem(pc + dc, 2)],
            dst_ref=came.at[pz, pc],
            send_sem=send_sem.at[n],
            recv_sem=recv_sem.at[n],
            device_id=peer(dz, dc),
            device_id_type=MESH,
        )
        copy.start()
        copies.append(copy)
    for copy in copies:
        copy.wait_recv()
    other = 1 - pc
    for w in range(out.shape[1]):
        mine = kept[w]
        for by in (1, 2, 3):
            mine = mine + came[lax.rem(pz + by, 4), pc, w].astype(F32)
        out[pc, w] = mine
        theirs = came[0, other, w].astype(F32)
        for z in (1, 2, 3):
            theirs = theirs + came[z, other, w].astype(F32)
        out[other, w] = theirs
    for copy in copies:
        copy.wait_send()


def column(sums, pz, pc):
    n = len(sums)
    blocks = jnp.stack([s.reshape(4, 2, 10, 16, 128) for s in sums], 2)
    kept = lax.dynamic_slice(blocks, (pz, pc, 0, 0, 0, 0), (1, 1, n, 10, 16, 128))[0, 0]
    vmem = pl.BlockSpec(memory_space=pltpu.VMEM)
    out = pl.pallas_call(
        column_kernel,
        out_shape=jax.ShapeDtypeStruct((2, n, 10, 16, 128), F32),
        in_specs=[vmem] * 2,
        out_specs=vmem,
        scratch_shapes=[pltpu.VMEM((4, 2, n, 10, 16, 128), BF), pltpu.SemaphoreType.DMA((7,)), pltpu.SemaphoreType.DMA((7,))],
        compiler_params=pltpu.CompilerParams(collective_id=3, has_side_effects=True),
        name="column",
    )(blocks.astype(BF), kept)
    return [out[:, w].transpose(1, 0, 2, 3).reshape(10, 4096) for w in range(n)]


def adamw(w, m, v, g):
    m = 0.9 * m + 0.1 * g
    v = 0.95 * v + 0.05 * g * g
    step = m * lax.rsqrt(v + 1e-8) + 0.1 * w
    return (w - 0.02 * step).astype(BF), m, v


def matmul(a, w):
    return jnp.dot(a, w, preferred_element_type=F32).astype(BF)


def normed(h):
    wide = h.astype(F32)
    scale = lax.rsqrt(jnp.mean(wide**2, -1, keepdims=True) + 1e-6)
    return (wide * scale).astype(BF)


def forward(h, wg, wu, wd):
    a = normed(h)
    gate = jnp.dot(a, wg, preferred_element_type=F32)
    up = jnp.dot(a, wu, preferred_element_type=F32)
    act = (jax.nn.silu(gate) * up).astype(BF)
    out = None if wd is None else h + matmul(act, wd)
    return out, (a, gate, up, act)


def across(a, w):
    return lax.dot_general(a, w, (((1,), (1,)), ((), ())), preferred_element_type=F32).astype(BF)


def product_of(a, b):
    return lax.dot_general(a, b, (((0,), (0,)), ((), ())), preferred_element_type=F32).astype(BF)


def backward(h, kept, by_out, wg, wu, wd, through):
    a, gate, up, act = kept
    by_act = across(by_out, wd).astype(F32)
    sig = jax.nn.sigmoid(gate)
    by_up = (by_act * (gate * sig)).astype(BF)
    by_gate = (by_act * up * (sig * (1 + gate * (1 - sig)))).astype(BF)
    pairs = [(a, by_gate), (a, by_up), (act, by_out)]
    if not through:
        return pairs, None
    by_a = across(by_gate, wg).astype(F32) + across(by_up, wu).astype(F32)
    _, back = jax.vjp(normed, h)
    return pairs, by_out + back(by_a.astype(BF))[0]


BESIDE = True


def solution(mesh):
    def body(x, dy, wg, wu, wd, mg, mu, md, vg, vu, vd):
        me = lax.axis_index("dp")
        px, py, pz, pc = place()
        h0, by_y = x[0], dy[0]
        h1, kept0 = forward(h0, wg[0], wu[0], wd[0])
        _, kept1 = forward(h1, wg[1], wu[1], None)
        pairs1, by_h1 = backward(h1, kept1, by_y, wg[1], wu[1], wd[1], True)
        pairs0, _ = backward(h0, kept0, by_h1, wg[0], wu[0], wd[0], False)
        by_1 = [product_of(*pair) for pair in pairs1]
        if BESIDE:
            sums1, by_0 = scatter(*by_1, [pairs0[2], pairs0[0], pairs0[1]], 1)
            by_0 = (by_0[1], by_0[2], by_0[0])
        else:
            sums1, _ = scatter(*by_1, [], 1)
            by_0 = [product_of(*pair) for pair in pairs0]
        sums0, _ = scatter(*by_0, [], 2)
        wide = column([sums0[0], sums1[0], sums0[1], sums1[1]], pz, pc)
        sums = {(0, 0): wide[0], (0, 1): wide[1], (1, 0): wide[2], (1, 1): wide[3], (2, 0): sums0[2], (2, 1): sums1[2]}
        new = {}
        for (i, n), g in sums.items():
            rows = g.shape[0]
            own = lax.dynamic_slice_in_dim((wg, wu, wd)[i][n], me * rows, rows, 0).astype(F32)
            new[i, n] = adamw(own, (mg, mu, md)[i][n], (vg, vu, vd)[i][n], g.astype(BF).astype(F32))
        stacked = [[jnp.stack([new[i, n][which] for n in range(2)]) for i in range(3)] for which in range(3)]
        owns = [stacked[0][0].reshape(2, 320, 128), stacked[0][1].reshape(2, 320, 128), stacked[0][2]]
        weights = [o.reshape(w.shape) for o, w in zip(gather(owns), (wg, wu, wd))]
        return (*weights, *stacked[1], *stacked[2])

    rows = P(None, "dp", None)
    return jax.shard_map(
        body,
        mesh=mesh,
        in_specs=(P("dp"), P("dp"), P(), P(), P(), *[rows] * 6),
        out_specs=(P(), P(), P(), *[rows] * 6),
        check_vma=False,
    )
```

```python
import functools

import jax
import jax.numpy as jnp
from jax import lax
from jax.experimental import pallas as pl
from jax.experimental.pallas import tpu as pltpu
from jax.sharding import PartitionSpec as P

MESH = pl.DeviceIdType.MESH
BF = jnp.bfloat16
F32 = jnp.float32


KINDS = ("zyx", "xzy", "yxz")


def neighbour(axis, by):
    me = lax.axis_index("dp")
    here = {"x": me // 32, "y": me // 8 % 4, "z": me // 2 % 4, "c": me % 2}
    size = 2 if axis == "c" else 4
    here[axis] = lax.rem(here[axis] + by, size)
    return {"dp": ((here["x"] * 4 + here["y"]) * 4 + here["z"]) * 2 + here["c"]}


PEERS = [(a, by) for a in "xyz" for by in (1, 2, 3)] + [("c", 1)]


def greet():
    barrier = pltpu.get_barrier_semaphore()
    for axis, by in PEERS:
        pl.semaphore_signal(barrier, inc=1, device_id=neighbour(axis, by), device_id_type=MESH)
    pl.semaphore_wait(barrier, len(PEERS))


def gather_kernel(own_g, own_u, own_d, out_g, out_u, out_d, local_sem, send_sem, recv_sem):
    me = lax.axis_index("dp")
    here = {"x": me // 32, "y": me // 8 % 4, "z": me // 2 % 4}
    c = me % 2
    greet()
    owns, outs = (own_g, own_u, own_d), (out_g, out_u, out_d)
    started = []

    def view(k, **where):
        spots = [where.get(a, slice(None)) for a in "xyz"]
        return outs[k].at[(slice(None), *spots, c)]

    def push(src, dst, axis, by):
        n = len(started)
        copy = pltpu.make_async_remote_copy(
            src_ref=src, dst_ref=dst, send_sem=send_sem.at[n], recv_sem=recv_sem.at[n], device_id=neighbour(axis, by), device_id_type=MESH
        )
        copy.start()
        started.append(copy)
        return copy

    first, second, third, relay, swaps = {}, {}, {}, {}, []
    keep = []
    for k in range(3):
        local = pltpu.make_async_copy(owns[k], view(k, **here), local_sem.at[k])
        local.start()
        keep.append(local)
        first[k] = [push(owns[k], view(k, **here), KINDS[k][0], by) for by in (1, 3, 2)]
    for k, (a, b, e) in enumerate(KINDS):
        keep[k].wait()
        for copy in first[k]:
            copy.wait_recv()
        line = view(k, **{b: here[b], e: here[e]})
        second[k] = [push(line, line, b, by) for by in (1, 3, 2)]
    for k, (a, b, e) in enumerate(KINDS):
        for copy in second[k]:
            copy.wait_recv()
        plane = view(k, **{e: here[e]})
        third[k] = [push(plane, plane, e, by) for by in (1, 3)]
        swaps.append(push(plane, plane, "c", 1))
    for k, (a, b, e) in enumerate(KINDS):
        relay[k] = []
        for copy, by, half in zip(third[k], (1, 3), (slice(0, 2), slice(2, 4))):
            copy.wait_recv()
            came = lax.rem(here[e] + 4 - by, 4)
            part = view(k, **{e: came, a: half})
            relay[k].append(push(part, part, e, by))
            plane = view(k, **{e: came})
            swaps.append(push(plane, plane, "c", 1))
    for k, (a, b, e) in enumerate(KINDS):
        for copy, half in zip(relay[k], (slice(0, 2), slice(2, 4))):
            copy.wait_recv()
            part = view(k, **{e: lax.rem(here[e] + 2, 4), a: half})
            swaps.append(push(part, part, "c", 1))
    for copy in swaps:
        copy.wait_recv()
    for copy in started:
        copy.wait_send()


COPIES = 3 * (3 + 3 + 2 + 2 + 5)


def gather(owns):
    shapes = [jax.ShapeDtypeStruct((2, 4, 4, 4, 2, *o.shape[1:]), o.dtype) for o in owns]
    return pl.pallas_call(
        gather_kernel,
        out_shape=shapes,
        in_specs=[pl.BlockSpec(memory_space=pltpu.VMEM)] * 3,
        out_specs=[pl.BlockSpec(memory_space=pl.ANY)] * 3,
        scratch_shapes=[pltpu.SemaphoreType.DMA((3,)), pltpu.SemaphoreType.DMA((COPIES,)), pltpu.SemaphoreType.DMA((COPIES,))],
        compiler_params=pltpu.CompilerParams(collective_id=0, has_side_effects=True),
        name="gather",
    )(*owns)


def place():
    me = lax.axis_index("dp")
    return me // 32, me // 8 % 4, me // 2 % 4, me % 2


def combine(dst, terms):
    *lead, rows, _ = dst.shape
    strips = rows // 16
    count = strips
    for n in lead:
        count *= n

    @pl.loop(0, count)
    def _(i):
        spot, q = [], i // strips
        for n in reversed(lead):
            spot.insert(0, q % n)
            q = q // n
        where = (*spot, pl.ds(pl.multiple_of(i % strips * 16, 16), 16), slice(None))
        out = terms[0][where].astype(F32)
        for t in terms[1:]:
            out = out + t[where].astype(F32)
        dst[where] = out.astype(dst.dtype)


def transposed_product(a, b, out, rows, columns):
    depth = a.shape[0]

    def tile(a_ref, b_ref, o_ref):
        o_ref[...] = lax.dot_general(a_ref[...], b_ref[...], (((0,), (0,)), ((), ())), preferred_element_type=F32).astype(BF)

    pltpu.emit_pipeline(
        tile,
        grid=(a.shape[1] // rows, b.shape[1] // columns),
        in_specs=[pl.BlockSpec((depth, rows), lambda i, j: (0, i)), pl.BlockSpec((depth, columns), lambda i, j: (0, j))],
        out_specs=[pl.BlockSpec((rows, columns), lambda i, j: (i, j))],
    )(a, b, out)


STEPS = (0, 1, 2)
SIDES = (0, 1)
BYS = (1, 3, 2)


def scatter_kernel(beside, g_g, g_u, g_d, *rest):
    ins, rest = rest[: 2 * beside], rest[2 * beside :]
    f_g, f_u, f_d = rest[:3]
    products, rest = rest[3 : 3 + beside], rest[3 + beside :]
    o_g, r_g, p_g, q_g, o_u, r_u, p_u, q_u, o_d, r_d, p_d, q_d, t_d, local_sem, send_sem, recv_sem = rest
    px, py, pz, pc = place()
    greet()
    started = []

    def push(src, dst, axis, by):
        n = len(started)
        copy = pltpu.make_async_remote_copy(
            src_ref=src, dst_ref=dst, send_sem=send_sem.at[n], recv_sem=recv_sem.at[n], device_id=neighbour(axis, by), device_id_type=MESH
        )
        copy.start()
        started.append(copy)
        return copy

    own, swapped = (o_g, o_u, o_d), (r_g, r_u, r_d)
    firsts, seconds = (p_g, p_u, p_d), (q_g, q_u, q_d)
    axes = ("xy", "yx", "zx")
    here = {"x": px, "y": py, "z": pz}

    def first_part(k, ref, t):
        return (ref.at[t], ref.at[:, t], ref.at[:, :, t])[k]

    def second_part(k, ref, t):
        return (ref.at[px, t], ref.at[t, py], ref.at[t, :, pz])[k]

    def chunk(k, c, t):
        if k == 2:
            return g_d.at[:, :, t, c]
        lanes = pl.ds(pl.multiple_of(c * 2048, 2048), 2048)
        return g_g.at[t, :, :, lanes] if k == 0 else g_u.at[:, t, :, lanes]

    swaps, loads = {}, {}
    for i, by in enumerate((2, 1, 3, 0)):
        for k in range(3):
            t = lax.rem(here[axes[k][0]] + by, 4)
            swaps[k, by] = push(chunk(k, 1 - pc, t), first_part(k, swapped[k], t), "c", 1)
            loads[k, by] = pltpu.make_async_copy(chunk(k, pc, t), first_part(k, own[k], t), local_sem.at[i * 3 + k])
            loads[k, by].start()

    def product(n):
        if n < beside:
            transposed_product(ins[2 * n], ins[2 * n + 1], products[n], *((512, 1280) if n == 0 else (640, 1024)))

    low, high = pl.ds(0, 2), pl.ds(2, 2)

    def part_of(k, ref, by, side):
        t = lax.rem(here[axes[k][0]] + by, 4)
        return (ref.at[t, side], ref.at[side, t], ref.at[side, :, t])[k]

    def add_and_push(k, by, side, more, slot, towards):
        part = part_of(k, own[k], by, side)
        combine(part, [part, part_of(k, swapped[k], by, side)] + more)
        return push(part, firsts[k].at[slot, side], axes[k][0], towards)

    relays, ring = {}, {k: [] for k in range(3)}
    for k in range(3):
        loads[k, 2].wait()
        swaps[k, 2].wait_recv()
        relays[k] = (add_and_push(k, 2, low, [], 2, 1), add_and_push(k, 2, high, [], 2, 3))
    for k in range(3):
        for by, side, slot in ((1, high, 0), (3, low, 1)):
            loads[k, by].wait()
            swaps[k, by].wait_recv()
            ring[k].append(add_and_push(k, by, side, [], slot, by))
    product(0)
    for k in range(3):
        for copy, by, side, slot in zip(relays[k], (1, 3), (low, high), (0, 1)):
            copy.wait_recv()
            ring[k].append(add_and_push(k, by, side, [firsts[k].at[2, side]], slot, by))
    product(1)
    for k in range(3):
        loads[k, 0].wait()
        swaps[k, 0].wait_recv()
    ring2 = {}
    for k in range(3):
        for copy in ring[k]:
            copy.wait_recv()
        ring2[k] = []
        for i, by in enumerate(BYS):
            t = lax.rem(here[axes[k][1]] + by, 4)
            part = second_part(k, own[k], t)
            combine(part, [part, second_part(k, swapped[k], t)] + [firsts[k].at[s, t] for s in SIDES])
            ring2[k].append(push(part, seconds[k].at[i], axes[k][1], by))
    product(2)
    last = []
    for copy in ring2[2]:
        copy.wait_recv()

    def terms_d(u):
        return [o_d.at[px, u, pz], r_d.at[px, u, pz]] + [p_d.at[s, px, u] for s in SIDES] + [q_d.at[s, u] for s in STEPS]

    for i, by in enumerate(BYS):
        u = lax.rem(py + by, 4)
        combine(o_d.at[px, u, pz], terms_d(u))
        last.append(push(o_d.at[px, u, pz], t_d.at[i], "y", by))
    for k, f in ((0, f_g), (1, f_u)):
        for copy in ring2[k]:
            copy.wait_recv()
        t = here[axes[k][1]]
        combine(f, [second_part(k, own[k], t), second_part(k, swapped[k], t)] + [firsts[k].at[s, t] for s in SIDES] + [seconds[k].at[s] for s in STEPS])
    for copy in last:
        copy.wait_recv()
    combine(f_d, terms_d(py) + [t_d.at[s] for s in STEPS])
    for copy in started:
        copy.wait_send()


def scatter(g_g, g_u, g_d, beside, identity):
    any_space, vmem = pl.BlockSpec(memory_space=pl.ANY), pl.BlockSpec(memory_space=pltpu.VMEM)
    copies = 12 + 18 + 9 + 3
    wide, tall = (4, 80, 2048), (4, 32, 1280)
    shapes = []
    for _ in range(2):
        shapes += [(4, *wide), (4, *wide), (3, *wide), (3, *wide[1:])]
    shapes += [(4, 4, *tall), (4, 4, *tall), (3, 4, *tall), (3, *tall), (3, *tall[1:])]
    operands = [t for pair in beside for t in pair]
    out = pl.pallas_call(
        functools.partial(scatter_kernel, len(beside)),
        out_shape=[jax.ShapeDtypeStruct((80, 2048), F32)] * 2
        + [jax.ShapeDtypeStruct((32, 1280), F32)]
        + [jax.ShapeDtypeStruct((a.shape[1], b.shape[1]), BF) for a, b in beside],
        in_specs=[any_space] * (3 + len(operands)),
        out_specs=[vmem] * 3 + [any_space] * len(beside),
        scratch_shapes=[pltpu.VMEM(s, BF) for s in shapes]
        + [pltpu.SemaphoreType.DMA((12,)), pltpu.SemaphoreType.DMA((copies,)), pltpu.SemaphoreType.DMA((copies,))],
        compiler_params=pltpu.CompilerParams(collective_id=identity, has_side_effects=True, vmem_limit_bytes=66_000_000),
        name=f"scatter{identity}",
    )(g_g.reshape(4, 4, 80, 4096), g_u.reshape(4, 4, 80, 4096), g_d.reshape(4, 4, 4, 2, 32, 1280), *operands)
    return out[:3], out[3:]


COLUMN = [(dz, dc) for dz in range(4) for dc in range(2) if dz or dc]


def column_kernel(parts, kept, out, came, send_sem, recv_sem):
    px, py, pz, pc = place()

    def peer(dz, dc):
        return {"dp": ((px * 4 + py) * 4 + lax.rem(pz + dz, 4)) * 2 + lax.rem(pc + dc, 2)}

    barrier = pltpu.get_barrier_semaphore()
    for dz, dc in COLUMN:
        pl.semaphore_signal(barrier, inc=1, device_id=peer(dz, dc), device_id_type=MESH)
    pl.semaphore_wait(barrier, len(COLUMN))
    copies = []
    for n, (dz, dc) in enumerate(COLUMN):
        copy = pltpu.make_async_remote_copy(
            src_ref=parts.at[lax.rem(pz + dz, 4), lax.rem(pc + dc, 2)],
            dst_ref=came.at[pz, pc],
            send_sem=send_sem.at[n],
            recv_sem=recv_sem.at[n],
            device_id=peer(dz, dc),
            device_id_type=MESH,
        )
        copy.start()
        copies.append(copy)
    for copy in copies:
        copy.wait_recv()
    other = 1 - pc
    for w in range(out.shape[1]):
        mine = kept[w]
        for by in (1, 2, 3):
            mine = mine + came[lax.rem(pz + by, 4), pc, w].astype(F32)
        out[pc, w] = mine
        theirs = came[0, other, w].astype(F32)
        for z in (1, 2, 3):
            theirs = theirs + came[z, other, w].astype(F32)
        out[other, w] = theirs
    for copy in copies:
        copy.wait_send()


def column(sums, pz, pc):
    n = len(sums)
    blocks = jnp.stack([s.reshape(4, 2, 10, 16, 128) for s in sums], 2)
    kept = lax.dynamic_slice(blocks, (pz, pc, 0, 0, 0, 0), (1, 1, n, 10, 16, 128))[0, 0]
    vmem = pl.BlockSpec(memory_space=pltpu.VMEM)
    out = pl.pallas_call(
        column_kernel,
        out_shape=jax.ShapeDtypeStruct((2, n, 10, 16, 128), F32),
        in_specs=[vmem] * 2,
        out_specs=vmem,
        scratch_shapes=[pltpu.VMEM((4, 2, n, 10, 16, 128), BF), pltpu.SemaphoreType.DMA((7,)), pltpu.SemaphoreType.DMA((7,))],
        compiler_params=pltpu.CompilerParams(collective_id=3, has_side_effects=True),
        name="column",
    )(blocks.astype(BF), kept)
    return [out[:, w].transpose(1, 0, 2, 3).reshape(10, 4096) for w in range(n)]


def adamw(w, m, v, g):
    m = 0.9 * m + 0.1 * g
    v = 0.95 * v + 0.05 * g * g
    step = m * lax.rsqrt(v + 1e-8) + 0.1 * w
    return (w - 0.02 * step).astype(BF), m, v


def matmul(a, w):
    return jnp.dot(a, w, preferred_element_type=F32).astype(BF)


def normed(h):
    wide = h.astype(F32)
    scale = lax.rsqrt(jnp.mean(wide**2, -1, keepdims=True) + 1e-6)
    return (wide * scale).astype(BF)


def forward(h, wg, wu, wd):
    a = normed(h)
    gate = jnp.dot(a, wg, preferred_element_type=F32)
    up = jnp.dot(a, wu, preferred_element_type=F32)
    act = (jax.nn.silu(gate) * up).astype(BF)
    out = None if wd is None else h + matmul(act, wd)
    return out, (a, gate, up, act)


def across(a, w):
    return lax.dot_general(a, w, (((1,), (1,)), ((), ())), preferred_element_type=F32).astype(BF)


def product_of(a, b):
    return lax.dot_general(a, b, (((0,), (0,)), ((), ())), preferred_element_type=F32).astype(BF)


def backward(h, kept, by_out, wg, wu, wd, through):
    a, gate, up, act = kept
    by_act = across(by_out, wd).astype(F32)
    sig = jax.nn.sigmoid(gate)
    by_up = (by_act * (gate * sig)).astype(BF)
    by_gate = (by_act * up * (sig * (1 + gate * (1 - sig)))).astype(BF)
    pairs = [(a, by_gate), (a, by_up), (act, by_out)]
    if not through:
        return pairs, None
    by_a = across(by_gate, wg).astype(F32) + across(by_up, wu).astype(F32)
    _, back = jax.vjp(normed, h)
    return pairs, by_out + back(by_a.astype(BF))[0]


BESIDE = True


def solution(mesh):
    def body(x, dy, wg, wu, wd, mg, mu, md, vg, vu, vd):
        me = lax.axis_index("dp")
        px, py, pz, pc = place()
        h0, by_y = x[0], dy[0]
        h1, kept0 = forward(h0, wg[0], wu[0], wd[0])
        _, kept1 = forward(h1, wg[1], wu[1], None)
        pairs1, by_h1 = backward(h1, kept1, by_y, wg[1], wu[1], wd[1], True)
        pairs0, _ = backward(h0, kept0, by_h1, wg[0], wu[0], wd[0], False)
        by_1 = [product_of(*pair) for pair in pairs1]
        if BESIDE:
            sums1, by_0 = scatter(*by_1, [pairs0[2], pairs0[0], pairs0[1]], 1)
            by_0 = (by_0[1], by_0[2], by_0[0])
        else:
            sums1, _ = scatter(*by_1, [], 1)
            by_0 = [product_of(*pair) for pair in pairs0]
        sums0, _ = scatter(*by_0, [], 2)
        wide = column([sums0[0], sums1[0], sums0[1], sums1[1]], pz, pc)
        sums = [jnp.stack(wide[:2]), jnp.stack(wide[2:]), jnp.stack([sums0[2], sums1[2]])]
        new = []
        for g, w, m, v in zip(sums, (wg, wu, wd), (mg, mu, md), (vg, vu, vd)):
            rows = g.shape[1]
            own = lax.dynamic_slice(w, (0, me * rows, 0), (2, rows, w.shape[2])).astype(F32)
            new.append(adamw(own, m, v, g.astype(BF).astype(F32)))
        stacked = [[t[which] for t in new] for which in range(3)]
        owns = [stacked[0][0].reshape(2, 320, 128), stacked[0][1].reshape(2, 320, 128), stacked[0][2]]
        weights = [o.reshape(w.shape) for o, w in zip(gather(owns), (wg, wu, wd))]
        return (*weights, *stacked[1], *stacked[2])

    rows = P(None, "dp", None)
    return jax.shard_map(
        body,
        mesh=mesh,
        in_specs=(P("dp"), P("dp"), P(), P(), P(), *[rows] * 6),
        out_specs=(P(), P(), P(), *[rows] * 6),
        check_vma=False,
    )
```

```python
import functools

import jax
import jax.numpy as jnp
from jax import lax
from jax.experimental import pallas as pl
from jax.experimental.pallas import tpu as pltpu
from jax.sharding import PartitionSpec as P

MESH = pl.DeviceIdType.MESH
BF = jnp.bfloat16
F32 = jnp.float32


KINDS = ("zyx", "xzy", "yxz")


def neighbour(axis, by):
    me = lax.axis_index("dp")
    here = {"x": me // 32, "y": me // 8 % 4, "z": me // 2 % 4, "c": me % 2}
    size = 2 if axis == "c" else 4
    here[axis] = lax.rem(here[axis] + by, size)
    return {"dp": ((here["x"] * 4 + here["y"]) * 4 + here["z"]) * 2 + here["c"]}


PEERS = [(a, by) for a in "xyz" for by in (1, 2, 3)] + [("c", 1)]


def across_column(dz, dc):
    px, py, pz, pc = place()
    return {"dp": ((px * 4 + py) * 4 + lax.rem(pz + dz, 4)) * 2 + lax.rem(pc + dc, 2)}


def greet(more=()):
    barrier = pltpu.get_barrier_semaphore()
    for device in [neighbour(axis, by) for axis, by in PEERS] + list(more):
        pl.semaphore_signal(barrier, inc=1, device_id=device, device_id_type=MESH)
    pl.semaphore_wait(barrier, len(PEERS) + len(more))


def gather_kernel(own_g, own_u, own_d, out_g, out_u, out_d, came_g, came_u, tall, wide_g, wide_u, local_sem, send_sem, recv_sem, column_send, column_recv):
    px, py, pz, c = place()
    here = {"x": px, "y": py, "z": pz}
    greet([across_column(dz, 1) for dz in (1, 2, 3)])
    owns, outs = (wide_g, wide_u, own_d), (out_g, out_u, out_d)
    started = []

    def view(k, **where):
        x, y, z = (where.get(a, slice(None)) for a in "xyz")
        if k == 2:
            return outs[k].at[:, x, y, z, c]
        first, count = c * 2048, 2048
        if "z" in where:
            first, count = (c * 2048 + z.start * 512, 1024) if isinstance(z, slice) else (c * 2048 + z * 512, 512)
        return outs[k].at[:, x, y, :, pl.ds(pl.multiple_of(first, 512), count)]

    def push(src, dst, axis, by):
        n = len(started)
        copy = pltpu.make_async_remote_copy(
            src_ref=src, dst_ref=dst, send_sem=send_sem.at[n], recv_sem=recv_sem.at[n], device_id=neighbour(axis, by), device_id_type=MESH
        )
        copy.start()
        started.append(copy)
        return copy

    column_copies = []
    for k, (own, came) in enumerate(((own_g, came_g), (own_u, came_u))):
        for n, (dz, dc) in enumerate(COLUMN):
            copy = pltpu.make_async_remote_copy(
                src_ref=own.at[lax.rem(pz + dz, 4), lax.rem(c + dc, 2)],
                dst_ref=came.at[pz, c],
                send_sem=column_send.at[k * 7 + n],
                recv_sem=column_recv.at[k * 7 + n],
                device_id=across_column(dz, dc),
                device_id_type=MESH,
            )
            copy.start()
            column_copies.append(copy)
        came[pz, c] = own[pz, c]
    first, second, third, relay, swaps = {}, {}, {}, {}, []
    keep = {}
    for k in (2, 0, 1):
        if k < 2:
            came = (came_g, came_u)[k]
            for copy in column_copies[k * 7 : k * 7 + 7]:
                copy.wait_recv()
            for z in range(4):
                for core in range(2):
                    tall[:, pl.ds(20 * z + 10 * core, 10), :] = came[z, core].astype(F32)
            owns[k][...] = tall[...].astype(BF)
        keep[k] = pltpu.make_async_copy(owns[k], view(k, **here), local_sem.at[k])
        keep[k].start()
        first[k] = [push(owns[k], view(k, **here), KINDS[k][0], by) for by in (1, 3, 2)]
    for k, (a, b, e) in enumerate(KINDS):
        keep[k].wait()
        for copy in first[k]:
            copy.wait_recv()
        line = view(k, **{b: here[b], e: here[e]})
        second[k] = [push(line, line, b, by) for by in (1, 3, 2)]
    for k, (a, b, e) in enumerate(KINDS):
        for copy in second[k]:
            copy.wait_recv()
        plane = view(k, **{e: here[e]})
        third[k] = [push(plane, plane, e, by) for by in (1, 3)]
        swaps.append(push(plane, plane, "c", 1))
    for k, (a, b, e) in enumerate(KINDS):
        relay[k] = []
        for copy, by, half in zip(third[k], (1, 3), (slice(0, 2), slice(2, 4))):
            copy.wait_recv()
            came = lax.rem(here[e] + 4 - by, 4)
            part = view(k, **{e: came, a: half})
            relay[k].append(push(part, part, e, by))
            plane = view(k, **{e: came})
            swaps.append(push(plane, plane, "c", 1))
    for k, (a, b, e) in enumerate(KINDS):
        for copy, half in zip(relay[k], (slice(0, 2), slice(2, 4))):
            copy.wait_recv()
            part = view(k, **{e: lax.rem(here[e] + 2, 4), a: half})
            swaps.append(push(part, part, "c", 1))
    for copy in swaps:
        copy.wait_recv()
    for copy in started + column_copies:
        copy.wait_send()


COPIES = 3 * (3 + 3 + 2 + 2 + 5)


def gather(own_g, own_u, own_d):
    wide = jax.ShapeDtypeStruct((2, 4, 4, 80, 4096), BF)
    return pl.pallas_call(
        gather_kernel,
        out_shape=[wide, wide, jax.ShapeDtypeStruct((2, 4, 4, 4, 2, 32, 1280), BF)],
        in_specs=[pl.BlockSpec(memory_space=pltpu.VMEM)] * 3,
        out_specs=[pl.BlockSpec(memory_space=pl.ANY)] * 3,
        scratch_shapes=[pltpu.VMEM((4, 2, 2, 10, 512), BF)] * 2
        + [pltpu.VMEM((2, 80, 512), F32)]
        + [pltpu.VMEM((2, 80, 512), BF)] * 2
        + [pltpu.SemaphoreType.DMA((n,)) for n in (3, COPIES, COPIES, 14, 14)],
        compiler_params=pltpu.CompilerParams(collective_id=0, has_side_effects=True),
        name="gather",
    )(own_g, own_u, own_d)


def place():
    me = lax.axis_index("dp")
    return me // 32, me // 8 % 4, me // 2 % 4, me % 2


def combine(dst, terms):
    *lead, rows, _ = dst.shape
    strips = rows // 16
    count = strips
    for n in lead:
        count *= n

    @pl.loop(0, count)
    def _(i):
        spot, q = [], i // strips
        for n in reversed(lead):
            spot.insert(0, q % n)
            q = q // n
        where = (*spot, pl.ds(pl.multiple_of(i % strips * 16, 16), 16), slice(None))
        out = terms[0][where].astype(F32)
        for t in terms[1:]:
            out = out + t[where].astype(F32)
        dst[where] = out.astype(dst.dtype)


def transposed_product(a, b, out, rows, columns):
    depth = a.shape[0]

    def tile(a_ref, b_ref, o_ref):
        o_ref[...] = lax.dot_general(a_ref[...], b_ref[...], (((0,), (0,)), ((), ())), preferred_element_type=F32).astype(BF)

    pltpu.emit_pipeline(
        tile,
        grid=(a.shape[1] // rows, b.shape[1] // columns),
        in_specs=[pl.BlockSpec((depth, rows), lambda i, j: (0, i)), pl.BlockSpec((depth, columns), lambda i, j: (0, j))],
        out_specs=[pl.BlockSpec((rows, columns), lambda i, j: (i, j))],
    )(a, b, out)


STEPS = (0, 1, 2)
SIDES = (0, 1)
BYS = (1, 3, 2)


def scatter_kernel(beside, g_g, g_u, g_d, *rest):
    ins, rest = rest[: 2 * beside], rest[2 * beside :]
    f_g, f_u, f_d = rest[:3]
    products, rest = rest[3 : 3 + beside], rest[3 + beside :]
    o_g, r_g, p_g, q_g, o_u, r_u, p_u, q_u, o_d, r_d, p_d, q_d, t_d, local_sem, send_sem, recv_sem = rest
    px, py, pz, pc = place()
    greet()
    started = []

    def push(src, dst, axis, by):
        n = len(started)
        copy = pltpu.make_async_remote_copy(
            src_ref=src, dst_ref=dst, send_sem=send_sem.at[n], recv_sem=recv_sem.at[n], device_id=neighbour(axis, by), device_id_type=MESH
        )
        copy.start()
        started.append(copy)
        return copy

    own, swapped = (o_g, o_u, o_d), (r_g, r_u, r_d)
    firsts, seconds = (p_g, p_u, p_d), (q_g, q_u, q_d)
    axes = ("xy", "yx", "zx")
    here = {"x": px, "y": py, "z": pz}

    def first_part(k, ref, t):
        return (ref.at[t], ref.at[:, t], ref.at[:, :, t])[k]

    def second_part(k, ref, t):
        return (ref.at[px, t], ref.at[t, py], ref.at[t, :, pz])[k]

    def chunk(k, c, t):
        if k == 2:
            return g_d.at[:, :, t, c]
        lanes = pl.ds(pl.multiple_of(c * 2048, 2048), 2048)
        return g_g.at[t, :, :, lanes] if k == 0 else g_u.at[:, t, :, lanes]

    swaps, loads = {}, {}
    for i, by in enumerate((2, 1, 3, 0)):
        for k in range(3):
            t = lax.rem(here[axes[k][0]] + by, 4)
            swaps[k, by] = push(chunk(k, 1 - pc, t), first_part(k, swapped[k], t), "c", 1)
            loads[k, by] = pltpu.make_async_copy(chunk(k, pc, t), first_part(k, own[k], t), local_sem.at[i * 3 + k])
            loads[k, by].start()

    def product(n):
        if n < beside:
            transposed_product(ins[2 * n], ins[2 * n + 1], products[n], *((512, 1280) if n == 0 else (640, 1024)))

    low, high = pl.ds(0, 2), pl.ds(2, 2)

    def part_of(k, ref, by, side):
        t = lax.rem(here[axes[k][0]] + by, 4)
        return (ref.at[t, side], ref.at[side, t], ref.at[side, :, t])[k]

    def add_and_push(k, by, side, more, slot, towards):
        part = part_of(k, own[k], by, side)
        combine(part, [part, part_of(k, swapped[k], by, side)] + more)
        return push(part, firsts[k].at[slot, side], axes[k][0], towards)

    relays, ring = {}, {k: [] for k in range(3)}
    for k in range(3):
        loads[k, 2].wait()
        swaps[k, 2].wait_recv()
        relays[k] = (add_and_push(k, 2, low, [], 2, 1), add_and_push(k, 2, high, [], 2, 3))
    for k in range(3):
        for by, side, slot in ((1, high, 0), (3, low, 1)):
            loads[k, by].wait()
            swaps[k, by].wait_recv()
            ring[k].append(add_and_push(k, by, side, [], slot, by))
    product(0)
    for k in range(3):
        for copy, by, side, slot in zip(relays[k], (1, 3), (low, high), (0, 1)):
            copy.wait_recv()
            ring[k].append(add_and_push(k, by, side, [firsts[k].at[2, side]], slot, by))
    product(1)
    for k in range(3):
        loads[k, 0].wait()
        swaps[k, 0].wait_recv()
    ring2 = {}
    for k in range(3):
        for copy in ring[k]:
            copy.wait_recv()
        ring2[k] = []
        for i, by in enumerate(BYS):
            t = lax.rem(here[axes[k][1]] + by, 4)
            part = second_part(k, own[k], t)
            combine(part, [part, second_part(k, swapped[k], t)] + [firsts[k].at[s, t] for s in SIDES])
            ring2[k].append(push(part, seconds[k].at[i], axes[k][1], by))
    product(2)
    last = []
    for copy in ring2[2]:
        copy.wait_recv()

    def terms_d(u):
        return [o_d.at[px, u, pz], r_d.at[px, u, pz]] + [p_d.at[s, px, u] for s in SIDES] + [q_d.at[s, u] for s in STEPS]

    for i, by in enumerate(BYS):
        u = lax.rem(py + by, 4)
        combine(o_d.at[px, u, pz], terms_d(u))
        last.append(push(o_d.at[px, u, pz], t_d.at[i], "y", by))
    for k, f in ((0, f_g), (1, f_u)):
        for copy in ring2[k]:
            copy.wait_recv()
        t = here[axes[k][1]]
        combine(f, [second_part(k, own[k], t), second_part(k, swapped[k], t)] + [firsts[k].at[s, t] for s in SIDES] + [seconds[k].at[s] for s in STEPS])
    for copy in last:
        copy.wait_recv()
    combine(f_d, terms_d(py) + [t_d.at[s] for s in STEPS])
    for copy in started:
        copy.wait_send()


def scatter(g_g, g_u, g_d, beside, identity):
    any_space, vmem = pl.BlockSpec(memory_space=pl.ANY), pl.BlockSpec(memory_space=pltpu.VMEM)
    copies = 12 + 18 + 9 + 3
    wide, tall = (4, 80, 2048), (4, 32, 1280)
    shapes = []
    for _ in range(2):
        shapes += [(4, *wide), (4, *wide), (3, *wide), (3, *wide[1:])]
    shapes += [(4, 4, *tall), (4, 4, *tall), (3, 4, *tall), (3, *tall), (3, *tall[1:])]
    operands = [t for pair in beside for t in pair]
    out = pl.pallas_call(
        functools.partial(scatter_kernel, len(beside)),
        out_shape=[jax.ShapeDtypeStruct((80, 2048), F32)] * 2
        + [jax.ShapeDtypeStruct((32, 1280), F32)]
        + [jax.ShapeDtypeStruct((a.shape[1], b.shape[1]), BF) for a, b in beside],
        in_specs=[any_space] * (3 + len(operands)),
        out_specs=[vmem] * 3 + [any_space] * len(beside),
        scratch_shapes=[pltpu.VMEM(s, BF) for s in shapes]
        + [pltpu.SemaphoreType.DMA((12,)), pltpu.SemaphoreType.DMA((copies,)), pltpu.SemaphoreType.DMA((copies,))],
        compiler_params=pltpu.CompilerParams(collective_id=identity, has_side_effects=True, vmem_limit_bytes=66_000_000),
        name=f"scatter{identity}",
    )(g_g.reshape(4, 4, 80, 4096), g_u.reshape(4, 4, 80, 4096), g_d.reshape(4, 4, 4, 2, 32, 1280), *operands)
    return out[:3], out[3:]


COLUMN = [(dz, dc) for dz in range(4) for dc in range(2) if dz or dc]


def column_kernel(parts, kept, out, came, send_sem, recv_sem):
    px, py, pz, pc = place()

    def peer(dz, dc):
        return {"dp": ((px * 4 + py) * 4 + lax.rem(pz + dz, 4)) * 2 + lax.rem(pc + dc, 2)}

    barrier = pltpu.get_barrier_semaphore()
    for dz, dc in COLUMN:
        pl.semaphore_signal(barrier, inc=1, device_id=peer(dz, dc), device_id_type=MESH)
    pl.semaphore_wait(barrier, len(COLUMN))
    copies = []
    for n, (dz, dc) in enumerate(COLUMN):
        copy = pltpu.make_async_remote_copy(
            src_ref=parts.at[lax.rem(pz + dz, 4), lax.rem(pc + dc, 2)],
            dst_ref=came.at[pz, pc],
            send_sem=send_sem.at[n],
            recv_sem=recv_sem.at[n],
            device_id=peer(dz, dc),
            device_id_type=MESH,
        )
        copy.start()
        copies.append(copy)
    for copy in copies:
        copy.wait_recv()
    other = 1 - pc
    for w in range(out.shape[1]):
        mine = kept[w]
        for by in (1, 2, 3):
            mine = mine + came[lax.rem(pz + by, 4), pc, w].astype(F32)
        out[pc, w] = mine
        theirs = came[0, other, w].astype(F32)
        for z in (1, 2, 3):
            theirs = theirs + came[z, other, w].astype(F32)
        out[other, w] = theirs
    for copy in copies:
        copy.wait_send()


def column(sums, pz, pc):
    n = len(sums)
    blocks = jnp.stack([s.reshape(4, 2, 10, 16, 128) for s in sums], 2)
    kept = lax.dynamic_slice(blocks, (pz, pc, 0, 0, 0, 0), (1, 1, n, 10, 16, 128))[0, 0]
    vmem = pl.BlockSpec(memory_space=pltpu.VMEM)
    out = pl.pallas_call(
        column_kernel,
        out_shape=jax.ShapeDtypeStruct((2, n, 10, 16, 128), F32),
        in_specs=[vmem] * 2,
        out_specs=vmem,
        scratch_shapes=[pltpu.VMEM((4, 2, n, 10, 16, 128), BF), pltpu.SemaphoreType.DMA((7,)), pltpu.SemaphoreType.DMA((7,))],
        compiler_params=pltpu.CompilerParams(collective_id=3, has_side_effects=True),
        name="column",
    )(blocks.astype(BF), kept)
    return [out[:, w].transpose(1, 0, 2, 3).reshape(10, 4096) for w in range(n)]


def adamw(w, m, v, g):
    m = 0.9 * m + 0.1 * g
    v = 0.95 * v + 0.05 * g * g
    step = m * lax.rsqrt(v + 1e-8) + 0.1 * w
    return (w - 0.02 * step).astype(BF), m, v


def matmul(a, w):
    return jnp.dot(a, w, preferred_element_type=F32).astype(BF)


def normed(h):
    wide = h.astype(F32)
    scale = lax.rsqrt(jnp.mean(wide**2, -1, keepdims=True) + 1e-6)
    return (wide * scale).astype(BF)


def forward(h, wg, wu, wd):
    a = normed(h)
    gate = jnp.dot(a, wg, preferred_element_type=F32)
    up = jnp.dot(a, wu, preferred_element_type=F32)
    act = (jax.nn.silu(gate) * up).astype(BF)
    out = None if wd is None else h + matmul(act, wd)
    return out, (a, gate, up, act)


def across(a, w):
    return lax.dot_general(a, w, (((1,), (1,)), ((), ())), preferred_element_type=F32).astype(BF)


def product_of(a, b):
    return lax.dot_general(a, b, (((0,), (0,)), ((), ())), preferred_element_type=F32).astype(BF)


def backward(h, kept, by_out, wg, wu, wd, through):
    a, gate, up, act = kept
    by_act = across(by_out, wd).astype(F32)
    sig = jax.nn.sigmoid(gate)
    by_up = (by_act * (gate * sig)).astype(BF)
    by_gate = (by_act * up * (sig * (1 + gate * (1 - sig)))).astype(BF)
    pairs = [(a, by_gate), (a, by_up), (act, by_out)]
    if not through:
        return pairs, None
    by_a = across(by_gate, wg).astype(F32) + across(by_up, wu).astype(F32)
    _, back = jax.vjp(normed, h)
    return pairs, by_out + back(by_a.astype(BF))[0]


BESIDE = True


def solution(mesh):
    def body(x, dy, wg, wu, wd, mg, mu, md, vg, vu, vd):
        me = lax.axis_index("dp")
        px, py, pz, pc = place()
        h0, by_y = x[0], dy[0]
        h1, kept0 = forward(h0, wg[0], wu[0], wd[0])
        _, kept1 = forward(h1, wg[1], wu[1], None)
        pairs1, by_h1 = backward(h1, kept1, by_y, wg[1], wu[1], wd[1], True)
        pairs0, _ = backward(h0, kept0, by_h1, wg[0], wu[0], wd[0], False)
        by_1 = [product_of(*pair) for pair in pairs1]
        if BESIDE:
            sums1, by_0 = scatter(*by_1, [pairs0[2], pairs0[0], pairs0[1]], 1)
            by_0 = (by_0[1], by_0[2], by_0[0])
        else:
            sums1, _ = scatter(*by_1, [], 1)
            by_0 = [product_of(*pair) for pair in pairs0]
        sums0, _ = scatter(*by_0, [], 2)
        wide = column([sums0[0], sums1[0], sums0[1], sums1[1]], pz, pc)
        sums = [jnp.stack(wide[:2]), jnp.stack(wide[2:]), jnp.stack([sums0[2], sums1[2]])]
        new = []
        for g, w, m, v in zip(sums, (wg, wu, wd), (mg, mu, md), (vg, vu, vd)):
            rows = g.shape[1]
            own = lax.dynamic_slice(w, (0, me * rows, 0), (2, rows, w.shape[2])).astype(F32)
            new.append(adamw(own, m, v, g.astype(BF).astype(F32)))
        stacked = [[t[which] for t in new] for which in range(3)]
        cut = [t.reshape(2, 10, 2, 4, 512).transpose(3, 2, 0, 1, 4) for t in stacked[0][:2]]
        weights = [o.reshape(w.shape) for o, w in zip(gather(*cut, stacked[0][2]), (wg, wu, wd))]
        return (*weights, *stacked[1], *stacked[2])

    rows = P(None, "dp", None)
    return jax.shard_map(
        body,
        mesh=mesh,
        in_specs=(P("dp"), P("dp"), P(), P(), P(), *[rows] * 6),
        out_specs=(P(), P(), P(), *[rows] * 6),
        check_vma=False,
    )
```
